32 devices in a mesh: prompt: 4 (over z), sample: 4 (over x, core), vocab: 2 (over y).
Axes of the slice: x: 2, y: 2, z: 4, core: 2. Of those that a mesh axis runs over, the one named last changes fastest.
Arguments:
- hidden: bfloat16 [4, 24, 3584], P('sample', ('prompt', 'vocab')), may hold values from -170 to 170
- unembed: bfloat16 [152064, 3584], P(('prompt', 'vocab')), may hold values from -1 to 1
- token_ids: int32 [4, 24], P('sample', ('prompt', 'vocab')), may hold values from 0 to 152063, as said below
- old_logp: float32 [4, 24], P('sample', ('prompt', 'vocab')), may hold values from -14 to -11
- ref_logp: float32 [4, 24], P('sample', ('prompt', 'vocab')), may hold values from -14 to -11
- loss_mask: int32 [4, 24], P('sample', ('prompt', 'vocab')), may hold values 0 or 1
- lengths: int32 [4, 4], P('prompt', 'sample'), may hold values from 1 to 6, as said below
- sample_valid: int32 [4, 4], P('prompt', 'sample'), may hold values 0 or 1
- rewards: int32 [4, 4], P('prompt', 'sample'), may hold values from -300 to 300
Outputs:
- token_logp: float32 [4, 24], P('sample', ('prompt', 'vocab'))
- token_loss: float32 [4, 24], P('sample', ('prompt', 'vocab'))
- advantages: float32 [4, 4], P('prompt', 'sample')
- loss: float32 [], replicated
The draws below stay inside these ranges and needn't reach their ends.
Inputs may be any that keep to these rules, and one draw needn't show every extreme that they name: `token_ids`: token ids name vocabulary entries. `lengths`: some response in every draw has length 6.
All inputs are finite; a program needn't handle non-finite values. No bound on the sum of `loss_mask` or of `sample_valid` on one device may be relied on, other than what follows from the above.
Results may differ from the reference program's by a relative error of at most 0.0003.
Values may be sent and summed in bfloat16 or wider, within the bound.
A program may use at most 192 MiB of HBM per device.

```python
import math
import jax
import jax.numpy as jnp
from jax import lax

D = 3584
VOCAB = 152064
PROMPTS = 4
SAMPLES = 4
LEN = 6
ROWS = 24
N_PROMPT = 4
N_VOCAB = 2


cluster_total = 64


mix_total = 16


def centre_table(key):
    return jnp.clip(jax.random.normal(jax.random.fold_in(key, 13), (cluster_total, D), jnp.float32), -5.5, 5.5)


def weight_row(key, centres, row_index):
    row_key = jax.random.fold_in(jax.random.fold_in(key, 11), row_index)
    first_pick = jax.random.randint(jax.random.fold_in(row_key, 1), (), 0, cluster_total)
    second_pick = jax.random.randint(jax.random.fold_in(row_key, 2), (), 0, cluster_total)
    cluster = jnp.minimum(first_pick, second_pick)
    noise_part = jnp.clip(jax.random.normal(jax.random.fold_in(row_key, 3), (D,), jnp.float32), -5.5, 5.5)
    size_factor = jnp.exp(jax.random.uniform(jax.random.fold_in(row_key, 4), (), jnp.float32, -0.25, 0.25))
    row_value = size_factor * (0.6 * centres[cluster] + 0.8 * noise_part) / math.sqrt(D)
    return jnp.clip(row_value, -1.0, 1.0)


def unembed_rows(key, indices):
    centres = centre_table(key)
    return jax.vmap(lambda row_index: weight_row(key, centres, row_index))(indices)


def label_table(key):
    return jax.random.randint(jax.random.fold_in(key, 23), (SAMPLES, ROWS), 0, VOCAB, dtype=jnp.int32)


def draw_unembed(key, part):
    return unembed_rows(key, jnp.arange(VOCAB, dtype=jnp.int32)).astype(jnp.bfloat16)


def draw_token_ids(key, part):
    return label_table(key)


def draw_hidden(key, part):
    flat_count = SAMPLES * ROWS
    noise_part = jnp.clip(jax.random.normal(jax.random.fold_in(key, 31), (flat_count, D), jnp.float32), -6.0, 6.0)
    picks = jax.random.randint(jax.random.fold_in(key, 43), (flat_count, mix_total), 0, VOCAB, dtype=jnp.int32)
    mix_weights = jax.random.uniform(jax.random.fold_in(key, 47), (flat_count, mix_total), jnp.float32, 3.0, 7.0)
    noise_scale = 0.5
    centres = centre_table(key)

    def mixture(item):
        row_picks, row_weights = item
        chosen_rows = jax.vmap(lambda row_index: weight_row(key, centres, row_index))(row_picks)
        return jnp.sum(row_weights[:, None] * chosen_rows, axis=0)
    mixed = lax.map(mixture, (picks, mix_weights))
    values = mixed + noise_scale * noise_part
    values = jnp.clip(values, -170.0, 170.0)
    return values.reshape(SAMPLES, ROWS, D).astype(jnp.bfloat16)


def draw_lengths(key, part):
    col_caps = jax.random.randint(jax.random.fold_in(key, 53), (SAMPLES,), 1, LEN + 1)
    raw_draw = jax.random.randint(jax.random.fold_in(key, 59), (PROMPTS, SAMPLES), 0, LEN)
    length_draw = 1 + raw_draw * col_caps[None, :] // LEN
    longest = jax.random.randint(jax.random.fold_in(key, 61), (), 0, SAMPLES)
    column = lax.broadcasted_iota(jnp.int32, (PROMPTS, SAMPLES), 1)
    row_line = lax.broadcasted_iota(jnp.int32, (PROMPTS, SAMPLES), 0)
    return jnp.where((column == longest) & (row_line == 0), LEN, length_draw).astype(jnp.int32)


def place_ends(drawn, key, smallest, largest):
    longest = drawn.shape.index(max(drawn.shape))
    spots = []
    for shift in (0, 1):
        where = [jax.random.randint(jax.random.fold_in(key, axis), (), 0, length) for axis, length in enumerate(drawn.shape)]
        where[longest] = (where[longest] + shift) % drawn.shape[longest]
        spots.append(tuple(where))
    return drawn.at[spots[0]].set(smallest).at[spots[1]].set(largest)


def level_of(own_key, dims, pieces, low, largest):
    factor_of = 1.0
    for axis_at, shards_of in pieces:
        steps = jax.random.uniform(jax.random.fold_in(jax.random.fold_in(own_key, 6), axis_at), (shards_of,), jnp.float32, low / len(pieces), largest / len(pieces))
        factor_of = factor_of * jnp.repeat(jnp.exp(steps), dims[axis_at] // shards_of).reshape((-1,) + (1,) * (len(dims) - 1 - axis_at))
    return factor_of


def setup_inputs(seed: int = 0) -> dict:
    arg_keys = jax.random.split(jax.random.key(seed), 10)
    hidden = draw_hidden(jax.random.fold_in(arg_keys[9], 71), 0)
    unembed = draw_unembed(jax.random.fold_in(arg_keys[9], 71), 0)
    token_ids = draw_token_ids(jax.random.fold_in(arg_keys[9], 71), 0)
    old_logp = jnp.clip(-14.0 + 3.0 * jax.random.uniform(arg_keys[3], (SAMPLES, ROWS), jnp.float32) ** level_of(arg_keys[3], (SAMPLES, ROWS), ((0, 4), (1, 8)), -0.2, 0.2), -14.0, -11.0)
    ref_logp = jnp.clip(-14.0 + 3.0 * jax.random.uniform(arg_keys[4], (SAMPLES, ROWS), jnp.float32) ** level_of(arg_keys[4], (SAMPLES, ROWS), ((0, 4), (1, 8)), -0.2, 0.2), -14.0, -11.0)
    loss_mask = place_ends((jax.random.randint(arg_keys[5], (SAMPLES, ROWS), 0, 8) < 7).astype(jnp.int32), jax.random.fold_in(arg_keys[5], 1), 0, 1)
    lengths = draw_lengths(jax.random.fold_in(arg_keys[9], 71), 0)
    sample_valid = place_ends((jax.random.randint(arg_keys[7], (PROMPTS, SAMPLES), 0, 8) < 7).astype(jnp.int32), jax.random.fold_in(arg_keys[7], 1), 0, 1)
    rewards = place_ends(jax.random.randint(arg_keys[8], (PROMPTS, SAMPLES), -300, 301), jax.random.fold_in(arg_keys[8], 1), -300, 300).astype(jnp.int32)
    return {"hidden": hidden, "unembed": unembed, "token_ids": token_ids, "old_logp": old_logp, "ref_logp": ref_logp, "loss_mask": loss_mask, "lengths": lengths, "sample_valid": sample_valid, "rewards": rewards}


clip_low = 0.8
clip_high = 1.2
dual_clip = 3.0
kl_weight = 0.04
reward_unit = 0.01
std_floor = 0.5
low_fill = -1e+30

def reference(hidden, unembed, token_ids, old_logp, ref_logp, loss_mask, lengths, sample_valid, rewards):
    samples, row_count, width = hidden.shape
    flat_count = samples * row_count
    flat_hidden = hidden.reshape(flat_count, width)
    flat_ids = token_ids.reshape(flat_count)
    shard_count = N_PROMPT * N_VOCAB
    shard_rows = unembed.shape[0] // shard_count
    shard_blocks = unembed.reshape(shard_count, shard_rows, width)

    def scan_step(totals, shard_item):
        run_peak, run_total, run_target = totals
        shard_block, shard_idx = shard_item
        logits = jnp.dot(flat_hidden, shard_block.T, preferred_element_type=jnp.float32)
        new_peak = jnp.maximum(run_peak, lax.optimization_barrier(jnp.max(logits, axis=1)))
        run_total = run_total * jnp.exp(run_peak - new_peak) + lax.optimization_barrier(jnp.sum(jnp.exp(logits - new_peak[:, None]), axis=1))
        column = shard_idx * shard_rows + lax.broadcasted_iota(jnp.int32, logits.shape, 1)
        run_target = run_target + lax.optimization_barrier(jnp.sum(jnp.where(column == flat_ids[:, None], logits, 0.0), axis=1))
        return ((new_peak, run_total, run_target), None)
    start_fill = (jnp.full((flat_count,), low_fill, jnp.float32), jnp.zeros((flat_count,), jnp.float32), jnp.zeros((flat_count,), jnp.float32))
    (run_peak, run_total, run_target), unused = lax.scan(scan_step, start_fill, (shard_blocks, jnp.arange(shard_count, dtype=jnp.int32)))
    raw_logp = (run_target - (run_peak + jnp.log(run_total))).reshape(samples, row_count)
    positions = lax.broadcasted_iota(jnp.int32, (samples, row_count), 1) % LEN
    length_rows = jnp.repeat(lengths.T, LEN, axis=1)
    valid_rows = jnp.repeat(sample_valid.T, LEN, axis=1)
    live_rows = (loss_mask == 1) & (positions < length_rows) & (valid_rows == 1)
    token_logp = jnp.where(live_rows, raw_logp, 0.0)
    valid_f = sample_valid.astype(jnp.float32)
    scores = rewards.astype(jnp.float32) * reward_unit
    group_count = lax.optimization_barrier(jnp.sum(valid_f, axis=1))
    first_moment = lax.optimization_barrier(jnp.sum(valid_f * scores, axis=1))
    second_moment = lax.optimization_barrier(jnp.sum(valid_f * scores * scores, axis=1))
    safe_count = jnp.maximum(group_count, 1.0)
    group_mean = first_moment / safe_count
    spread = jnp.sqrt(jnp.maximum(second_moment / safe_count - group_mean * group_mean, 0.0))
    advantages = valid_f * (scores - group_mean[:, None]) / jnp.maximum(spread, std_floor)[:, None]
    adv_rows = jnp.repeat(advantages.T, LEN, axis=1)
    prob_ratio = jnp.exp(raw_logp - old_logp)
    gain_side = adv_rows * jnp.minimum(prob_ratio, clip_high)
    loss_side = jnp.maximum(adv_rows * jnp.maximum(prob_ratio, clip_low), dual_clip * adv_rows)
    objective = jnp.where(adv_rows >= 0.0, gain_side, loss_side)
    log_gap = ref_logp - raw_logp
    kl_term = jnp.exp(log_gap) - log_gap - 1.0
    token_loss = jnp.where(live_rows, kl_weight * kl_term - objective, 0.0)
    live_total = jnp.sum(live_rows.astype(jnp.float32))
    loss = jnp.sum(token_loss) / jnp.maximum(live_total, 1.0)
    return (token_logp, token_loss, advantages, loss)
```

```python
import functools

import jax
import jax.numpy as jnp
from jax import lax
from jax.experimental import pallas as pl
from jax.experimental.pallas import tpu as pltpu
from jax.sharding import PartitionSpec as P

clip_low = 0.8
clip_high = 1.2
dual_clip = 3.0
kl_weight = 0.04
reward_unit = 0.01
std_floor = 0.5


def combined_all(value, axis, join):
    pieces = jax.tree.map(lambda part: lax.all_gather(part, axis), value)
    head = jax.tree.map(lambda part: part[0], pieces)
    tail = jax.tree.map(lambda part: part[1:], pieces)
    total, _ = lax.scan(lambda total, slab: (join(total, slab), None), head, tail)
    return total


def shard_stats(row_block, labels, weight, vocab_start):
    logits = lax.dot_general(
        row_block, weight, (((1,), (1,)), ((), ())), preferred_element_type=jnp.float32
    )
    local_peak = jnp.max(logits, axis=1)
    exp_total = jnp.sum(jnp.exp(logits - local_peak[:, None]), axis=1)
    column = vocab_start + lax.broadcasted_iota(jnp.int32, logits.shape, 1)
    target = jnp.sum(jnp.where(column == labels[:, None], logits, 0.0), axis=1)
    return (local_peak, exp_total, target)


def merge_pairs(first_part, second_part):
    peak_one, total_one, target_one = first_part
    peak_two, total_two, target_two = second_part
    joined_peak = jnp.maximum(peak_one, peak_two)
    joined_total = total_one * jnp.exp(peak_one - joined_peak) + total_two * jnp.exp(
        peak_two - joined_peak
    )
    return (joined_peak, joined_total, target_one + target_two)


def local_plain(
    hidden, unembed, token_ids, old_logp, ref_logp, loss_mask, lengths, sample_valid, rewards
):
    samples, local_rows, width = hidden.shape
    vocab_rows = unembed.shape[0]
    vocab_start = lax.axis_index(("prompt", "vocab")) * vocab_rows
    positions = lax.axis_index("vocab") * local_rows + lax.broadcasted_iota(
        jnp.int32, (samples, local_rows), 1
    )
    live_rows = (loss_mask == 1) & (positions < lengths.T) & (sample_valid.T == 1)
    live_float = live_rows.astype(jnp.float32)
    valid_f = sample_valid.astype(jnp.float32)
    scores = rewards.astype(jnp.float32) * reward_unit
    group_count, first_moment, second_moment = lax.psum(
        (
            jnp.sum(valid_f, axis=1),
            jnp.sum(valid_f * scores, axis=1),
            jnp.sum(valid_f * scores * scores, axis=1),
        ),
        "sample",
    )
    safe_count = jnp.maximum(group_count, 1.0)
    group_mean = first_moment / safe_count
    spread = jnp.sqrt(jnp.maximum(second_moment / safe_count - group_mean * group_mean, 0.0))
    advantages = valid_f * (scores - group_mean[:, None]) / jnp.maximum(spread, std_floor)[:, None]
    part_hidden = lax.all_gather(hidden, ("prompt", "vocab"), axis=1, tiled=True)
    part_ids = lax.all_gather(token_ids, ("prompt", "vocab"), axis=1, tiled=True)
    piece_rows = part_hidden.shape[1]
    piece_stats = shard_stats(
        part_hidden.reshape(samples * piece_rows, width),
        part_ids.reshape(samples * piece_rows),
        unembed,
        vocab_start,
    )
    peak_new = piece_stats[0].reshape(samples, piece_rows)
    total_new = piece_stats[1].reshape(samples, piece_rows)
    target_new = piece_stats[2].reshape(samples, piece_rows)
    row_top, total_all, target_all = combined_all(
        (peak_new, total_new, target_new), ("prompt", "vocab"), merge_pairs
    )
    own_start = lax.axis_index(("prompt", "vocab")) * local_rows

    def own_rows(values):
        return lax.dynamic_slice_in_dim(values, own_start, local_rows, 1)

    raw_logp = own_rows(target_all) - (own_rows(row_top) + jnp.log(own_rows(total_all)))
    token_logp = jnp.where(live_rows, raw_logp, 0.0)
    adv_rows = advantages.T
    prob_ratio = jnp.exp(raw_logp - old_logp)
    gain_side = adv_rows * jnp.minimum(prob_ratio, clip_high)
    loss_side = jnp.maximum(adv_rows * jnp.maximum(prob_ratio, clip_low), dual_clip * adv_rows)
    objective = jnp.where(adv_rows >= 0.0, gain_side, loss_side)
    log_gap = ref_logp - raw_logp
    kl_term = jnp.exp(log_gap) - log_gap - 1.0
    token_loss = jnp.where(live_rows, kl_weight * kl_term - objective, 0.0)
    loss_part = jnp.sum(token_loss)
    loss_total, live_total = lax.psum(
        (loss_part, jnp.sum(live_float)), ("prompt", "sample", "vocab")
    )
    loss = loss_total / jnp.maximum(live_total, 1.0)
    return (token_logp, token_loss, advantages, loss)


lanes = 128
tile_rows = 16
MESH = pl.DeviceIdType.MESH


def chunk_bounds(width):
    step = 512
    first = step if width % step == 0 else width
    bounds = [(0, first)]
    while bounds[-1][1] < width:
        start = bounds[-1][1]
        bounds.append((start, min(start + 2 * step, width)))
    return bounds


def row_blocks(rows):
    for count in (9, 8, 10, 12, 6, 4, 3, 2, 1):
        if rows % count == 0 and (rows // count) % tile_rows == 0:
            return count
    return 0


def merge_slots(tiles):
    peak = functools.reduce(jnp.maximum, [tile[0:1] for tile in tiles])
    total = sum(tile[1:2] * jnp.exp(tile[0:1] - peak) for tile in tiles)
    target = sum(tile[2:3] for tile in tiles)
    return peak, total, target


def fused_kernel(
    dims, hid, weight, ids, old, ref, mask, lengths, valid, rewards,
    logp_out, loss_out, adv_out, mean_out,
    wbuf, zrows, wide, held, acc, fz, fx, fc, sz, sx, sc,
    wsem, zs, zr, xs, xr, cs, cr, fzs, fzr, fxs, fxr, fcs, fcr, szs, szr, sxs, sxr, scs, scr,
):
    np_, ns, nv, local_rows, slot_rows, sub, width, blocks = dims
    hi_count = ns // 2
    bounds = chunk_bounds(width)
    z = lax.axis_index("prompt")
    s = lax.axis_index("sample")
    y = lax.axis_index("vocab")
    hi, lo = s // 2, s % 2
    block_rows = sub // blocks

    w_start = pl.multiple_of(s * sub, tile_rows)
    w_copies = []
    for b in range(blocks):
        copy = pltpu.make_async_copy(
            weight.at[pl.ds(w_start + b * block_rows, block_rows), :],
            wbuf.at[pl.ds(b * block_rows, block_rows), :],
            wsem.at[b],
        )
        copy.start()
        w_copies.append(copy)

    z_peers = [(lax.rem(z + j, np_), s, y) for j in range(1, np_)]
    plane = [(a, b) for a in range(hi_count) for b in range(nv) if (a, b) != (0, 0)]
    x_peers = [(z, lax.rem(hi + a, hi_count) * 2 + lo, lax.rem(y + b, nv)) for a, b in plane]
    c_peer = (z, hi * 2 + (1 - lo), y)
    barrier = pltpu.get_barrier_semaphore()
    peers = z_peers + x_peers + [c_peer]
    for peer in peers:
        pl.semaphore_signal(barrier, inc=1, device_id=peer, device_id_type=MESH)

    half = hi_count * nv
    group_own = hi * nv + y
    group = lo * half + group_own
    base_lane = group * tile_rows + z * slot_rows

    lane = lax.broadcasted_iota(jnp.int32, (8, lanes), 1)
    field = lax.broadcasted_iota(jnp.int32, (8, lanes), 0)
    valid_s = valid[0, 0]
    valid_f = valid_s.astype(jnp.float32)
    score = rewards[0, 0].astype(jnp.float32) * reward_unit
    inside = (lane >= base_lane) & (lane < base_lane + slot_rows)
    tile = jnp.where(inside & (field == 4), valid_f, 0.0)
    tile = jnp.where(inside & (field == 5), score, tile)
    for r in range(local_rows):
        here = lane == base_lane + r
        is_live = (
            (mask[0, r] == 1) & (y * local_rows + r < lengths[0, 0]) & (valid_s == 1)
        )
        live = jnp.where(is_live, 1.0, 0.0)
        tile = jnp.where(here & (field == 0), ids[0, r].astype(jnp.float32), tile)
        tile = jnp.where(here & (field == 1), old[0, r], tile)
        tile = jnp.where(here & (field == 2), ref[0, r], tile)
        tile = jnp.where(here & (field == 3), live, tile)
    fz[z] = tile
    wide[...] = jnp.zeros_like(wide)

    pl.semaphore_wait(barrier, len(peers))

    def remote(src, dst, send, recv, peer):
        copy = pltpu.make_async_remote_copy(
            src_ref=src, dst_ref=dst, send_sem=send, recv_sem=recv,
            device_id=peer, device_id_type=MESH,
        )
        copy.start()
        return copy

    def spread(buf, own, send, recv, to):
        return [
            remote(buf.at[own], buf.at[own], send.at[j], recv.at[j], peer)
            for j, peer in enumerate(to)
        ]

    def wait_all(copies):
        for copy in copies:
            copy.wait()

    z_copies = []
    for c, (k0, k1) in enumerate(bounds):
        cols = pl.ds(k0, k1 - k0)
        z_copies.append([
            remote(hid.at[0, :, cols], zrows.at[z, :, cols], zs.at[c, j], zr.at[c, j], peer)
            for j, peer in enumerate(z_peers)
        ])
        if c == 0:
            f_z = spread(fz, z, fzs, fzr, z_peers)
    zrows[z] = hid[0]

    x_copies = []
    for c, (k0, k1) in enumerate(bounds):
        cols = pl.ds(k0, k1 - k0)
        wait_all(z_copies[c])
        for p in range(np_):
            wide[p * slot_rows : p * slot_rows + local_rows, k0:k1] = zrows[p, :, k0:k1].astype(
                jnp.float32
            )
        held[group, :, k0:k1] = wide[:, k0:k1].astype(held.dtype)
        x_copies.append([
            remote(
                held.at[group, :, cols], held.at[group, :, cols], xs.at[c, j], xr.at[c, j], peer
            )
            for j, peer in enumerate(x_peers)
        ])
        if c == 0:
            wait_all(f_z)
            fx[group_own] = sum(fz[p] for p in range(np_))
            f_x = spread(fx, group_own, fxs, fxr, x_peers)

    def swap(c):
        k0, k1 = bounds[c]
        wait_all(x_copies[c])
        view = held.at[pl.ds(lo * half, half), :, pl.ds(k0, k1 - k0)]
        return remote(view, view, cs.at[c], cr.at[c], c_peer)

    def product(rows, k0, k1):
        rhs = held[:, :, k0:k1].reshape(lanes, k1 - k0)
        return lax.dot_general(
            wbuf[rows, k0:k1], rhs, (((1,), (1,)), ((), ())),
            preferred_element_type=jnp.float32,
        )

    first_id = ((z * nv + y) * (ns * sub) + s * sub).astype(jnp.float32)
    row_pos = lax.broadcasted_iota(jnp.int32, (block_rows, lanes), 0).astype(jnp.float32)
    pending = swap(0)
    carry = None
    for c, (k0, k1) in enumerate(bounds):
        pending.wait()
        if c + 1 < len(bounds):
            pending = swap(c + 1)
        if c == 0:
            for b in range(blocks):
                w_copies[b].wait()
                rows = pl.ds(b * block_rows, block_rows)
                acc[rows, :] = product(rows, k0, k1)
            wait_all(f_x)
            fc[lo] = sum(fx[g] for g in range(half))
            f_c = spread(fc, lo, fcs, fcr, [c_peer])
        elif c + 1 < len(bounds):

            @pl.loop(0, blocks)
            def _(b):
                rows = pl.ds(pl.multiple_of(b * block_rows, tile_rows), block_rows)
                acc[rows, :] += product(rows, k0, k1)
        else:
            wait_all(f_c)
            fields = fc[0] + fc[1]
            wanted = fields[0:1] - first_id

            def last(b, carry):
                peak, total, target = carry
                rows = pl.ds(pl.multiple_of(b * block_rows, tile_rows), block_rows)
                logits = acc[rows, :] + product(rows, k0, k1)
                shift = wanted - (b * block_rows).astype(jnp.float32)
                hit = jnp.where(row_pos == shift, logits, 0.0).reshape(-1, 8, lanes)
                cube = logits.reshape(-1, 8, lanes)
                peak_new = jnp.maximum(peak, jnp.max(cube, axis=0))
                total = total * jnp.exp(peak - peak_new) + jnp.sum(
                    jnp.exp(cube - peak_new[None]), axis=0
                )
                return peak_new, total, target + jnp.sum(hit, axis=0)

            start = (
                jnp.full((8, lanes), -1e30, jnp.float32),
                jnp.zeros((8, lanes), jnp.float32),
                jnp.zeros((8, lanes), jnp.float32),
            )
            peak8, total8, target8 = lax.fori_loop(0, blocks, last, start)
    peak = jnp.max(peak8, axis=0, keepdims=True)
    total = jnp.sum(total8 * jnp.exp(peak8 - peak), axis=0, keepdims=True)
    target = jnp.sum(target8, axis=0, keepdims=True)

    def pack(peak, total, target):
        return jnp.where(field == 0, peak, jnp.where(field == 1, total, target))

    sc[lo] = pack(peak, total, target)
    wait_all(spread(sc, lo, scs, scr, [c_peer]))
    sx[group_own] = pack(*merge_slots([sc[g] for g in range(2)]))
    wait_all(spread(sx, group_own, sxs, sxr, x_peers))
    sz[z] = pack(*merge_slots([sx[g] for g in range(half)]))
    wait_all(spread(sz, z, szs, szr, z_peers))
    peak, total, target = merge_slots([sz[p] for p in range(np_)])

    old_row, ref_row, live_row = fields[1:2], fields[2:3], fields[3:4] > 0.5
    valid_row, score_row = fields[4:5], fields[5:6]

    def over_samples(row):
        row8 = jnp.broadcast_to(row, (8, lanes))
        out = row8
        for j in range(1, ns):
            out = out + pltpu.roll(row8, j * nv * tile_rows, 1)
        return out[0:1]

    safe_count = jnp.maximum(over_samples(valid_row), 1.0)
    group_mean = over_samples(valid_row * score_row) / safe_count
    second = over_samples(valid_row * score_row * score_row) / safe_count
    spread_row = jnp.sqrt(jnp.maximum(second - group_mean * group_mean, 0.0))
    adv = valid_row * (score_row - group_mean) / jnp.maximum(spread_row, std_floor)
    raw = target - (peak + jnp.log(total))
    logp = jnp.where(live_row, raw, 0.0)
    ratio = jnp.exp(raw - old_row)
    gain = adv * jnp.minimum(ratio, clip_high)
    down = jnp.maximum(adv * jnp.maximum(ratio, clip_low), dual_clip * adv)
    objective = jnp.where(adv >= 0.0, gain, down)
    gap = ref_row - raw
    kl = jnp.exp(gap) - gap - 1.0
    loss = jnp.where(live_row, kl_weight * kl - objective, 0.0)
    loss_sum = jnp.sum(loss, axis=1, keepdims=True)
    live_sum = jnp.sum(jnp.where(live_row, 1.0, 0.0), axis=1, keepdims=True)
    mean_out[...] = loss_sum / jnp.maximum(live_sum, 1.0)

    mixed = jnp.where(field == 0, logp, jnp.where(field == 1, loss, adv))
    mine = pltpu.roll(mixed, lax.rem(lanes - base_lane, lanes), 1)
    logp_out[...] = mine[0:1, 0:local_rows]
    loss_out[...] = mine[1:2, 0:local_rows]
    adv_out[...] = mine[2:3, 0:1]


def local_fused(dims, *args):
    np_, ns, nv, local_rows, slot_rows, sub, width, blocks = dims
    half = ns // 2 * nv
    n_chunks = len(chunk_bounds(width))
    dma = pltpu.SemaphoreType.DMA
    vmem = pl.BlockSpec(memory_space=pltpu.VMEM)
    smem = pl.BlockSpec(memory_space=pltpu.SMEM)
    tile = lambda n: pltpu.VMEM((n, 8, lanes), jnp.float32)
    pair = lambda *shape: [dma(shape), dma(shape)]
    outs = pl.pallas_call(
        functools.partial(fused_kernel, dims),
        out_shape=(
            jax.ShapeDtypeStruct((1, local_rows), jnp.float32),
            jax.ShapeDtypeStruct((1, local_rows), jnp.float32),
            jax.ShapeDtypeStruct((1, 1), jnp.float32),
            jax.ShapeDtypeStruct((1, 1), jnp.float32),
        ),
        in_specs=[vmem, pl.BlockSpec(memory_space=pl.ANY)] + [smem] * 7,
        out_specs=(vmem,) * 4,
        scratch_shapes=[
            pltpu.VMEM((sub, width), jnp.bfloat16),
            pltpu.VMEM((np_, local_rows, width), jnp.bfloat16),
            pltpu.VMEM((tile_rows, width), jnp.float32),
            pltpu.VMEM((2 * half, tile_rows, width), jnp.bfloat16),
            pltpu.VMEM((sub, lanes), jnp.float32),
            tile(np_), tile(half), tile(2), tile(np_), tile(half), tile(2),
            dma((blocks,)),
            *pair(n_chunks, np_ - 1), *pair(n_chunks, half - 1), *pair(n_chunks),
            *pair(np_ - 1), *pair(half - 1), *pair(1),
            *pair(np_ - 1), *pair(half - 1), *pair(1),
        ],
        compiler_params=pltpu.CompilerParams(
            collective_id=0, has_side_effects=True, vmem_limit_bytes=60 * 1024 * 1024
        ),
    )(*args)
    return outs[0], outs[1], outs[2], outs[3].reshape(())


def local(hidden, unembed, *rest, shape):
    np_, ns, nv = shape
    samples, local_rows, width = hidden.shape
    vocab_rows = unembed.shape[0]
    slot_rows = tile_rows // np_ if tile_rows % np_ == 0 else 0
    sub = vocab_rows // ns
    blocks = row_blocks(sub)
    fits = (
        samples == 1
        and rest[-1].shape == (1, 1)
        and np_ > 1
        and ns % 2 == 0
        and ns // 2 * nv > 1
        and ns * nv * tile_rows == lanes
        and local_rows <= slot_rows
        and vocab_rows % ns == 0
        and blocks > 0
        and width % 512 == 0
        and width > 1024
        and sub * (width * 2 + lanes * 4) <= 48 * 1024 * 1024
    )
    if not fits:
        return local_plain(hidden, unembed, *rest)
    dims = (np_, ns, nv, local_rows, slot_rows, sub, width, blocks)
    return local_fused(dims, hidden, unembed, *rest)


def solution(mesh):
    in_specs = (
        P("sample", ("prompt", "vocab"), None),
        P(("prompt", "vocab"), None),
        P("sample", ("prompt", "vocab")),
        P("sample", ("prompt", "vocab")),
        P("sample", ("prompt", "vocab")),
        P("sample", ("prompt", "vocab")),
        P("prompt", "sample"),
        P("prompt", "sample"),
        P("prompt", "sample"),
    )
    out_specs = (
        P("sample", ("prompt", "vocab")),
        P("sample", ("prompt", "vocab")),
        P("prompt", "sample"),
        P(),
    )
    shape = (mesh.shape["prompt"], mesh.shape["sample"], mesh.shape["vocab"])
    body = functools.partial(local, shape=shape)
    return jax.shard_map(body, mesh=mesh, in_specs=in_specs, out_specs=out_specs, check_vma=False)
```

```python
import functools

import jax
import jax.numpy as jnp
from jax import lax
from jax.experimental import pallas as pl
from jax.experimental.pallas import tpu as pltpu
from jax.sharding import PartitionSpec as P

clip_low = 0.8
clip_high = 1.2
dual_clip = 3.0
kl_weight = 0.04
reward_unit = 0.01
std_floor = 0.5


def combined_all(value, axis, join):
    pieces = jax.tree.map(lambda part: lax.all_gather(part, axis), value)
    head = jax.tree.map(lambda part: part[0], pieces)
    tail = jax.tree.map(lambda part: part[1:], pieces)
    total, _ = lax.scan(lambda total, slab: (join(total, slab), None), head, tail)
    return total


def shard_stats(row_block, labels, weight, vocab_start):
    logits = lax.dot_general(
        row_block, weight, (((1,), (1,)), ((), ())), preferred_element_type=jnp.float32
    )
    local_peak = jnp.max(logits, axis=1)
    exp_total = jnp.sum(jnp.exp(logits - local_peak[:, None]), axis=1)
    column = vocab_start + lax.broadcasted_iota(jnp.int32, logits.shape, 1)
    target = jnp.sum(jnp.where(column == labels[:, None], logits, 0.0), axis=1)
    return (local_peak, exp_total, target)


def merge_pairs(first_part, second_part):
    peak_one, total_one, target_one = first_part
    peak_two, total_two, target_two = second_part
    joined_peak = jnp.maximum(peak_one, peak_two)
    joined_total = total_one * jnp.exp(peak_one - joined_peak) + total_two * jnp.exp(
        peak_two - joined_peak
    )
    return (joined_peak, joined_total, target_one + target_two)


def local_plain(
    hidden, unembed, token_ids, old_logp, ref_logp, loss_mask, lengths, sample_valid, rewards
):
    samples, local_rows, width = hidden.shape
    vocab_rows = unembed.shape[0]
    vocab_start = lax.axis_index(("prompt", "vocab")) * vocab_rows
    positions = lax.axis_index("vocab") * local_rows + lax.broadcasted_iota(
        jnp.int32, (samples, local_rows), 1
    )
    live_rows = (loss_mask == 1) & (positions < lengths.T) & (sample_valid.T == 1)
    live_float = live_rows.astype(jnp.float32)
    valid_f = sample_valid.astype(jnp.float32)
    scores = rewards.astype(jnp.float32) * reward_unit
    group_count, first_moment, second_moment = lax.psum(
        (
            jnp.sum(valid_f, axis=1),
            jnp.sum(valid_f * scores, axis=1),
            jnp.sum(valid_f * scores * scores, axis=1),
        ),
        "sample",
    )
    safe_count = jnp.maximum(group_count, 1.0)
    group_mean = first_moment / safe_count
    spread = jnp.sqrt(jnp.maximum(second_moment / safe_count - group_mean * group_mean, 0.0))
    advantages = valid_f * (scores - group_mean[:, None]) / jnp.maximum(spread, std_floor)[:, None]
    part_hidden = lax.all_gather(hidden, ("prompt", "vocab"), axis=1, tiled=True)
    part_ids = lax.all_gather(token_ids, ("prompt", "vocab"), axis=1, tiled=True)
    piece_rows = part_hidden.shape[1]
    piece_stats = shard_stats(
        part_hidden.reshape(samples * piece_rows, width),
        part_ids.reshape(samples * piece_rows),
        unembed,
        vocab_start,
    )
    peak_new = piece_stats[0].reshape(samples, piece_rows)
    total_new = piece_stats[1].reshape(samples, piece_rows)
    target_new = piece_stats[2].reshape(samples, piece_rows)
    row_top, total_all, target_all = combined_all(
        (peak_new, total_new, target_new), ("prompt", "vocab"), merge_pairs
    )
    own_start = lax.axis_index(("prompt", "vocab")) * local_rows

    def own_rows(values):
        return lax.dynamic_slice_in_dim(values, own_start, local_rows, 1)

    raw_logp = own_rows(target_all) - (own_rows(row_top) + jnp.log(own_rows(total_all)))
    token_logp = jnp.where(live_rows, raw_logp, 0.0)
    adv_rows = advantages.T
    prob_ratio = jnp.exp(raw_logp - old_logp)
    gain_side = adv_rows * jnp.minimum(prob_ratio, clip_high)
    loss_side = jnp.maximum(adv_rows * jnp.maximum(prob_ratio, clip_low), dual_clip * adv_rows)
    objective = jnp.where(adv_rows >= 0.0, gain_side, loss_side)
    log_gap = ref_logp - raw_logp
    kl_term = jnp.exp(log_gap) - log_gap - 1.0
    token_loss = jnp.where(live_rows, kl_weight * kl_term - objective, 0.0)
    loss_part = jnp.sum(token_loss)
    loss_total, live_total = lax.psum(
        (loss_part, jnp.sum(live_float)), ("prompt", "sample", "vocab")
    )
    loss = loss_total / jnp.maximum(live_total, 1.0)
    return (token_logp, token_loss, advantages, loss)


lanes = 128
tile_rows = 16
MESH = pl.DeviceIdType.MESH


def chunk_bounds(width):
    step = 512
    first = step if width % step == 0 else width
    bounds = [(0, first)]
    while bounds[-1][1] < width:
        start = bounds[-1][1]
        bounds.append((start, min(start + 2 * step, width)))
    return bounds


def row_blocks(rows):
    for count in (9, 8, 10, 12, 6, 4, 3, 2, 1):
        if rows % count == 0 and (rows // count) % tile_rows == 0:
            return count
    return 0


def merge_slots(tiles):
    peak = functools.reduce(jnp.maximum, [tile[0:1] for tile in tiles])
    total = sum(tile[1:2] * jnp.exp(tile[0:1] - peak) for tile in tiles)
    target = sum(tile[2:3] for tile in tiles)
    return peak, total, target


def fused_kernel(
    dims, hid, weight, ids, old, ref, mask, lengths, valid, rewards,
    out,
    wbuf, zrows, wide, held, acc, fz, fx, fc, sz, sx,
    wsem, zs, zr, xs, xr, cs, cr, fzs, fzr, fxs, fxr, fcs, fcr, szs, szr, sxs, sxr,
):
    np_, ns, nv, local_rows, slot_rows, sub, width, blocks = dims
    hi_count = ns // 2
    bounds = chunk_bounds(width)
    z = lax.axis_index("prompt")
    s = lax.axis_index("sample")
    y = lax.axis_index("vocab")
    hi, lo = s // 2, s % 2
    block_rows = sub // blocks

    w_start = pl.multiple_of(s * sub, tile_rows)
    w_copies = []
    for b in range(blocks):
        copy = pltpu.make_async_copy(
            weight.at[pl.ds(w_start + b * block_rows, block_rows), :],
            wbuf.at[pl.ds(b * block_rows, block_rows), :],
            wsem.at[b],
        )
        copy.start()
        w_copies.append(copy)

    z_peers = [(lax.rem(z + j, np_), s, y) for j in range(1, np_)]
    plane = [(a, b) for a in range(hi_count) for b in range(nv) if (a, b) != (0, 0)]
    x_peers = [(z, lax.rem(hi + a, hi_count) * 2 + lo, lax.rem(y + b, nv)) for a, b in plane]
    c_peer = (z, hi * 2 + (1 - lo), y)
    barrier = pltpu.get_barrier_semaphore()
    far_peers = [(pz, ps + 1 - 2 * lo, py) for pz, ps, py in x_peers]
    block_peers = [c_peer] + x_peers + far_peers
    peers = z_peers + block_peers
    for peer in peers:
        pl.semaphore_signal(barrier, inc=1, device_id=peer, device_id_type=MESH)

    half = hi_count * nv
    group_own = hi * nv + y
    group = lo * half + group_own
    base_lane = group * tile_rows + z * slot_rows

    lane = lax.broadcasted_iota(jnp.int32, (8, lanes), 1)
    field = lax.broadcasted_iota(jnp.int32, (8, lanes), 0)
    valid_s = valid[0, 0]
    valid_f = valid_s.astype(jnp.float32)
    score = rewards[0, 0].astype(jnp.float32) * reward_unit
    inside = (lane >= base_lane) & (lane < base_lane + slot_rows)
    tile = jnp.where(inside & (field == 4), valid_f, 0.0)
    tile = jnp.where(inside & (field == 5), score, tile)
    for r in range(local_rows):
        here = lane == base_lane + r
        is_live = (
            (mask[0, r] == 1) & (y * local_rows + r < lengths[0, 0]) & (valid_s == 1)
        )
        live = jnp.where(is_live, 1.0, 0.0)
        tile = jnp.where(here & (field == 0), ids[0, r].astype(jnp.float32), tile)
        tile = jnp.where(here & (field == 1), old[0, r], tile)
        tile = jnp.where(here & (field == 2), ref[0, r], tile)
        tile = jnp.where(here & (field == 3), live, tile)
    fz[z] = tile
    wide[...] = jnp.zeros_like(wide)

    pl.semaphore_wait(barrier, len(peers))

    def remote(src, dst, send, recv, peer):
        copy = pltpu.make_async_remote_copy(
            src_ref=src, dst_ref=dst, send_sem=send, recv_sem=recv,
            device_id=peer, device_id_type=MESH,
        )
        copy.start()
        return copy

    def spread(buf, own, send, recv, to):
        return [
            remote(buf.at[own], buf.at[own], send.at[j], recv.at[j], peer)
            for j, peer in enumerate(to)
        ]

    def wait_all(copies):
        for copy in copies:
            copy.wait()

    z_copies = []
    for c, (k0, k1) in enumerate(bounds):
        cols = pl.ds(k0, k1 - k0)
        z_copies.append([
            remote(hid.at[0, :, cols], zrows.at[z, :, cols], zs.at[c, j], zr.at[c, j], peer)
            for j, peer in enumerate(z_peers)
        ])
        if c == 0:
            f_z = spread(fz, z, fzs, fzr, z_peers)
    zrows[z] = hid[0]

    x_copies = []
    for c, (k0, k1) in enumerate(bounds):
        cols = pl.ds(k0, k1 - k0)
        wait_all(z_copies[c])
        for p in range(np_):
            wide[p * slot_rows : p * slot_rows + local_rows, k0:k1] = zrows[p, :, k0:k1].astype(
                jnp.float32
            )
        held[group, :, k0:k1] = wide[:, k0:k1].astype(held.dtype)
        x_copies.append([
            remote(
                held.at[group, :, cols], held.at[group, :, cols], xs.at[c, j], xr.at[c, j], peer
            )
            for j, peer in enumerate(x_peers)
        ])
        if c == 0:
            wait_all(f_z)
            fx[group_own] = sum(fz[p] for p in range(np_))
            f_x = spread(fx, group_own, fxs, fxr, x_peers)

    def swap(c):
        k0, k1 = bounds[c]
        wait_all(x_copies[c])
        view = held.at[pl.ds(lo * half, half), :, pl.ds(k0, k1 - k0)]
        return remote(view, view, cs.at[c], cr.at[c], c_peer)

    def product(rows, k0, k1):
        rhs = held[:, :, k0:k1].reshape(lanes, k1 - k0)
        return lax.dot_general(
            wbuf[rows, k0:k1], rhs, (((1,), (1,)), ((), ())),
            preferred_element_type=jnp.float32,
        )

    first_id = ((z * nv + y) * (ns * sub) + s * sub).astype(jnp.float32)
    row_pos = lax.broadcasted_iota(jnp.int32, (block_rows, lanes), 0).astype(jnp.float32)
    pending = swap(0)
    carry = None
    for c, (k0, k1) in enumerate(bounds):
        pending.wait()
        if c == 0:
            for b in range(blocks):
                if b == blocks // 2:
                    pending = swap(1)
                w_copies[b].wait()
                rows = pl.ds(b * block_rows, block_rows)
                acc[rows, :] = product(rows, k0, k1)
            wait_all(f_x)
            fc[lo] = sum(fx[g] for g in range(half))
            f_c = spread(fc, lo, fcs, fcr, [c_peer])
        elif c + 1 < len(bounds):

            def middle(b):
                rows = pl.ds(pl.multiple_of(b * block_rows, tile_rows), block_rows)
                acc[rows, :] += product(rows, k0, k1)

            pl.loop(0, blocks // 2)(middle)
            pending = swap(c + 1)
            pl.loop(blocks // 2, blocks)(middle)
        else:
            wait_all(f_c)
            fields = fc[0] + fc[1]
            wanted = fields[0:1] - first_id

            def last(b, carry):
                peak, total, target = carry
                rows = pl.ds(pl.multiple_of(b * block_rows, tile_rows), block_rows)
                logits = acc[rows, :] + product(rows, k0, k1)
                shift = wanted - (b * block_rows).astype(jnp.float32)
                hit = jnp.where(row_pos == shift, logits, 0.0).reshape(-1, 8, lanes)
                cube = logits.reshape(-1, 8, lanes)
                peak_new = jnp.maximum(peak, jnp.max(cube, axis=0))
                total = total * jnp.exp(peak - peak_new) + jnp.sum(
                    jnp.exp(cube - peak_new[None]), axis=0
                )
                return peak_new, total, target + jnp.sum(hit, axis=0)

            start = (
                jnp.full((8, lanes), -1e30, jnp.float32),
                jnp.zeros((8, lanes), jnp.float32),
                jnp.zeros((8, lanes), jnp.float32),
            )
            peak8, total8, target8 = lax.fori_loop(0, blocks, last, start)
    peak = jnp.max(peak8, axis=0, keepdims=True)
    total = jnp.sum(total8 * jnp.exp(peak8 - peak), axis=0, keepdims=True)
    target = jnp.sum(target8, axis=0, keepdims=True)

    def pack(peak, total, target):
        return jnp.where(field == 0, peak, jnp.where(field == 1, total, target))

    sx[group] = pack(peak, total, target)
    wait_all(spread(sx, group, sxs, sxr, block_peers))
    sz[z] = pack(*merge_slots([sx[g] for g in range(2 * half)]))
    wait_all(spread(sz, z, szs, szr, z_peers))
    peak, total, target = merge_slots([sz[p] for p in range(np_)])

    old_row, ref_row, live_row = fields[1:2], fields[2:3], fields[3:4] > 0.5
    valid_row, score_row = fields[4:5], fields[5:6]

    def over_samples(row):
        row8 = jnp.broadcast_to(row, (8, lanes))
        summed = row8
        for j in range(1, ns):
            summed = summed + pltpu.roll(row8, j * nv * tile_rows, 1)
        return summed[0:1]

    safe_count = jnp.maximum(over_samples(valid_row), 1.0)
    group_mean = over_samples(valid_row * score_row) / safe_count
    second = over_samples(valid_row * score_row * score_row) / safe_count
    spread_row = jnp.sqrt(jnp.maximum(second - group_mean * group_mean, 0.0))
    adv = valid_row * (score_row - group_mean) / jnp.maximum(spread_row, std_floor)
    raw = target - (peak + jnp.log(total))
    logp = jnp.where(live_row, raw, 0.0)
    ratio = jnp.exp(raw - old_row)
    gain = adv * jnp.minimum(ratio, clip_high)
    down = jnp.maximum(adv * jnp.maximum(ratio, clip_low), dual_clip * adv)
    objective = jnp.where(adv >= 0.0, gain, down)
    gap = ref_row - raw
    kl = jnp.exp(gap) - gap - 1.0
    loss = jnp.where(live_row, kl_weight * kl - objective, 0.0)
    loss_sum = jnp.sum(loss, axis=1, keepdims=True)
    live_sum = jnp.sum(jnp.where(live_row, 1.0, 0.0), axis=1, keepdims=True)
    mean = loss_sum / jnp.maximum(live_sum, 1.0)

    mixed = jnp.where(field == 0, logp, jnp.where(field == 1, loss, adv))
    mine = pltpu.roll(mixed, lax.rem(lanes - base_lane, lanes), 1)
    out[...] = jnp.where(field == 3, mean, mine)


def local_fused(dims, *args):
    np_, ns, nv, local_rows, slot_rows, sub, width, blocks = dims
    half = ns // 2 * nv
    n_chunks = len(chunk_bounds(width))
    dma = pltpu.SemaphoreType.DMA
    vmem = pl.BlockSpec(memory_space=pltpu.VMEM)
    smem = pl.BlockSpec(memory_space=pltpu.SMEM)
    tile = lambda n: pltpu.VMEM((n, 8, lanes), jnp.float32)
    pair = lambda *shape: [dma(shape), dma(shape)]
    out = pl.pallas_call(
        functools.partial(fused_kernel, dims),
        out_shape=jax.ShapeDtypeStruct((8, lanes), jnp.float32),
        in_specs=[vmem, pl.BlockSpec(memory_space=pl.ANY)] + [smem] * 7,
        out_specs=vmem,
        scratch_shapes=[
            pltpu.VMEM((sub, width), jnp.bfloat16),
            pltpu.VMEM((np_, local_rows, width), jnp.bfloat16),
            pltpu.VMEM((tile_rows, width), jnp.float32),
            pltpu.VMEM((2 * half, tile_rows, width), jnp.bfloat16),
            pltpu.VMEM((sub, lanes), jnp.float32),
            tile(np_), tile(half), tile(2), tile(np_), tile(2 * half),
            dma((blocks,)),
            *pair(n_chunks, np_ - 1), *pair(n_chunks, half - 1), *pair(n_chunks),
            *pair(np_ - 1), *pair(half - 1), *pair(1),
            *pair(np_ - 1), *pair(2 * half - 1),
        ],
        compiler_params=pltpu.CompilerParams(
            collective_id=0, has_side_effects=True, vmem_limit_bytes=60 * 1024 * 1024
        ),
    )(*args)
    return out[0:1, :local_rows], out[1:2, :local_rows], out[2:3, :1], out[3, 0]


def local(hidden, unembed, *rest, shape):
    np_, ns, nv = shape
    samples, local_rows, width = hidden.shape
    vocab_rows = unembed.shape[0]
    slot_rows = tile_rows // np_ if tile_rows % np_ == 0 else 0
    sub = vocab_rows // ns
    blocks = row_blocks(sub)
    fits = (
        samples == 1
        and rest[-1].shape == (1, 1)
        and np_ > 1
        and ns % 2 == 0
        and ns // 2 * nv > 1
        and ns * nv * tile_rows == lanes
        and local_rows <= slot_rows
        and vocab_rows % ns == 0
        and blocks > 0
        and width % 512 == 0
        and width > 1024
        and sub * (width * 2 + lanes * 4) <= 48 * 1024 * 1024
    )
    if not fits:
        return local_plain(hidden, unembed, *rest)
    dims = (np_, ns, nv, local_rows, slot_rows, sub, width, blocks)
    return local_fused(dims, hidden, unembed, *rest)


def solution(mesh):
    in_specs = (
        P("sample", ("prompt", "vocab"), None),
        P(("prompt", "vocab"), None),
        P("sample", ("prompt", "vocab")),
        P("sample", ("prompt", "vocab")),
        P("sample", ("prompt", "vocab")),
        P("sample", ("prompt", "vocab")),
        P("prompt", "sample"),
        P("prompt", "sample"),
        P("prompt", "sample"),
    )
    out_specs = (
        P("sample", ("prompt", "vocab")),
        P("sample", ("prompt", "vocab")),
        P("prompt", "sample"),
        P(),
    )
    shape = (mesh.shape["prompt"], mesh.shape["sample"], mesh.shape["vocab"])
    body = functools.partial(local, shape=shape)
    return jax.shard_map(body, mesh=mesh, in_specs=in_specs, out_specs=out_specs, check_vma=False)
```
